32 devices in a mesh: seq: 16 (over z, y, core), head: 2 (over x).
Axes of the slice: x: 2, y: 2, z: 4, core: 2. Of those that a mesh axis runs over, the one named last changes fastest.
Arguments:
- tokens: bfloat16 [8192, 2048], P('seq', 'head'), may hold values from -200 to 200
- norm_gain: float32 [2, 2048], replicated, may hold values from 0.25 to 1.75
- w_query: bfloat16 [2, 2048, 2048], P(None, None, 'head'), may hold values from -0.35 to 0.35
- key_projection_weight: bfloat16 [2, 2048, 512], P(None, None, 'head'), may hold values from -0.35 to 0.35
- value_projection_weight: bfloat16 [2, 2048, 512], P(None, None, 'head'), may hold values from -0.125 to 0.125
- w_out: bfloat16 [2, 2048, 2048], P(None, 'head'), may hold values from -0.125 to 0.125
- counts: int32 [16], replicated, may hold values from 128 to 512
Outputs:
- hidden_out: bfloat16 [8192, 2048], P('seq', 'head')
The draws below stay inside these ranges and needn't reach their ends.
Inputs may be any that keep to these rules, and one draw needn't show every extreme that they name: The first counts[b] tokens of block b of 512 positions are valid keys; the rest of the block is padding that no query uses as a key.
All inputs are finite; a program needn't handle non-finite values.
Results may differ from the reference program's by a relative error of at most 0.02.
The reference program's roundings to bfloat16 on the way count: a program that leaves them out, or rounds other values in their place, can miss the bound.
Values may be sent and summed in bfloat16 or wider, within the bound.
A program may use at most 128 MiB of HBM per device.

```python
import math
import jax
import jax.numpy as jnp
from jax import lax

MODEL_WIDTH = 2048
QUERY_HEAD_COUNT = 16
KEY_VALUE_HEADS = 4
HEAD_SIZE = 128
WINDOW = 4096
LAYER_COUNT = 2
BLOCK_TOKENS = 512
BLOCKS = 16
SEQUENCE_TOKENS = 8192
N_HEAD = 2


def sample_projection(key, salt, columns):
    scale_value = 1.6 / math.sqrt(MODEL_WIDTH)
    inner = jax.random.fold_in(key, salt)
    sampled_values = scale_value * jax.random.normal(inner, (LAYER_COUNT, MODEL_WIDTH, columns), jnp.float32)
    return jnp.clip(sampled_values, -0.35, 0.35)


def draw_w_query(key, part):
    sampled_values = sample_projection(key, 101, QUERY_HEAD_COUNT * HEAD_SIZE)
    return sampled_values.astype(jnp.bfloat16)


def draw_key_projection_weight(key, part):
    sampled_values = sample_projection(key, 102, KEY_VALUE_HEADS * HEAD_SIZE)
    return sampled_values.astype(jnp.bfloat16)


def draw_tokens(key, part):
    inner = jax.random.fold_in(key, 201)
    values = jnp.clip(jax.random.normal(inner, (SEQUENCE_TOKENS, MODEL_WIDTH), jnp.float32), -6.0, 6.0)
    return values.astype(jnp.bfloat16)


def set_ends(entries, rng, smallest, top_value):
    index_at = [jax.random.randint(jax.random.fold_in(rng, axis), (), 0, length) for axis, length in enumerate(entries.shape)]
    longest = entries.shape.index(max(entries.shape))
    next_to = index_at[:longest] + [(index_at[longest] + 1) % entries.shape[longest]] + index_at[longest + 1:]
    return entries.at[tuple(index_at)].set(smallest).at[tuple(next_to)].set(top_value)


def levels(key, dims, pieces, smallest, top_value):
    factor_of, own = 1.0, jax.random.fold_in(key, 6)
    for dim, shards_of in pieces:
        steps = jnp.exp(jax.random.uniform(jax.random.fold_in(own, dim), (shards_of,), jnp.float32, smallest / len(pieces), top_value / len(pieces)))
        factor_of = factor_of * jnp.repeat(steps, dims[dim] // shards_of).reshape([-1 if axis == dim else 1 for axis in range(len(dims))])
    return factor_of


def normal_values(stream_key, dims, width, most, pieces=(), kind=jnp.bfloat16):
    result = width * jax.random.normal(stream_key, dims, jnp.float32)
    if pieces:
        result = result * levels(stream_key, dims, pieces, -0.22, 0.18)
    return jnp.clip(result, -most, most).astype(kind)


def setup_inputs(seed: int = 0) -> dict:
    keys = jax.random.split(jax.random.key(seed), 8)
    return {
        "tokens": draw_tokens(jax.random.fold_in(keys[7], 71), 0),
        "norm_gain": jnp.clip(1.0 + 0.15 * jax.random.normal(keys[1], (LAYER_COUNT, MODEL_WIDTH), jnp.float32), 0.25, 1.75),
        "w_query": draw_w_query(jax.random.fold_in(keys[7], 71), 0),
        "key_projection_weight": draw_key_projection_weight(jax.random.fold_in(keys[7], 71), 0),
        "value_projection_weight": normal_values(keys[4], (LAYER_COUNT, MODEL_WIDTH, KEY_VALUE_HEADS * HEAD_SIZE), MODEL_WIDTH ** -0.5, 0.125, ((2, 2),)),
        "w_out": normal_values(keys[5], (LAYER_COUNT, QUERY_HEAD_COUNT * HEAD_SIZE, MODEL_WIDTH), (QUERY_HEAD_COUNT * HEAD_SIZE) ** -0.5, 0.125, ((1, 2),)),
        "counts": set_ends(jax.random.randint(keys[6], (BLOCKS,), BLOCK_TOKENS // 4, BLOCK_TOKENS + 1), jax.random.fold_in(keys[6], 1), BLOCK_TOKENS // 4, BLOCK_TOKENS).astype(jnp.int32),
    }


norm_epsilon = 1e-05
rope_base = 10000.0

def rms_norm(hidden, gain_row):
    widened = hidden.astype(jnp.float32)
    mean_square = lax.optimization_barrier(jnp.mean(widened * widened, axis=-1, keepdims=True))
    scaled = widened * lax.rsqrt(mean_square + norm_epsilon) * gain_row.astype(jnp.float32)
    return scaled.astype(jnp.bfloat16)

def apply_rotary_embedding(projected, token_positions, head_count):
    row_total = projected.shape[0]
    shaped = projected.reshape(row_total, head_count, HEAD_SIZE)
    half_dim = HEAD_SIZE // 2
    inverse = jnp.power(jnp.float32(rope_base), -2.0 * jnp.arange(half_dim, dtype=jnp.float32) / HEAD_SIZE)
    angles = token_positions.astype(jnp.float32)[:, None] * inverse[None, :]
    cosine_table = jnp.cos(angles)[:, None, :]
    sine_table = jnp.sin(angles)[:, None, :]
    first_half = shaped[..., :half_dim]
    second_half = shaped[..., half_dim:]
    rotated = jnp.concatenate([first_half * cosine_table - second_half * sine_table, second_half * cosine_table + first_half * sine_table], axis=-1)
    return rotated.astype(jnp.bfloat16)

def key_validity(key_positions, counts):
    key_block = jnp.floor_divide(key_positions, BLOCK_TOKENS)
    within_block = key_positions - key_block * BLOCK_TOKENS
    block_count = counts[jnp.clip(key_block, 0, BLOCKS - 1)]
    return (key_positions >= 0) & (within_block < block_count)

def attend(queries, key_rows_full, value_rows_full, counts):
    span_blocks = WINDOW // BLOCK_TOKENS
    group_length = QUERY_HEAD_COUNT // KEY_VALUE_HEADS
    padding_rows = span_blocks * BLOCK_TOKENS
    key_rows_padded = jnp.concatenate([jnp.zeros((padding_rows, KEY_VALUE_HEADS, HEAD_SIZE), jnp.bfloat16), key_rows_full], axis=0)
    value_rows_padded = jnp.concatenate([jnp.zeros((padding_rows, KEY_VALUE_HEADS, HEAD_SIZE), jnp.bfloat16), value_rows_full], axis=0)
    key_length = (span_blocks + 1) * BLOCK_TOKENS
    scale_factor = 1.0 / math.sqrt(HEAD_SIZE)

    def one_block(block_index):
        first_row = block_index * BLOCK_TOKENS
        block_of_queries = lax.dynamic_slice_in_dim(queries, first_row, BLOCK_TOKENS, 0)
        key_block = lax.dynamic_slice_in_dim(key_rows_padded, first_row, key_length, 0)
        value_block = lax.dynamic_slice_in_dim(value_rows_padded, first_row, key_length, 0)
        query_positions = first_row + jnp.arange(BLOCK_TOKENS, dtype=jnp.int32)
        key_positions = first_row - padding_rows + jnp.arange(key_length, dtype=jnp.int32)
        allowed = key_validity(key_positions, counts)[None, :]
        allowed = allowed & (key_positions[None, :] <= query_positions[:, None])
        allowed = allowed & (query_positions[:, None] - key_positions[None, :] < WINDOW)
        query_broad = block_of_queries.astype(jnp.float32).reshape(BLOCK_TOKENS, KEY_VALUE_HEADS, group_length, HEAD_SIZE)
        key_wide = key_block.astype(jnp.float32)
        scores = jnp.einsum('tkgd,lkd->kgtl', query_broad, key_wide, precision=lax.Precision.HIGHEST) * scale_factor
        scores = jnp.where(allowed[None, None], scores, -jnp.inf)
        largest = lax.optimization_barrier(jnp.max(scores, axis=-1, keepdims=True))
        weights = jnp.exp(scores - largest)
        weights = (weights / lax.optimization_barrier(jnp.sum(weights, axis=-1, keepdims=True))).astype(jnp.bfloat16)
        blended = jnp.einsum('kgtl,lkd->tkgd', weights.astype(jnp.float32), value_block.astype(jnp.float32), precision=lax.Precision.HIGHEST)
        return blended.astype(jnp.bfloat16).reshape(BLOCK_TOKENS, QUERY_HEAD_COUNT * HEAD_SIZE)
    outputs = lax.map(one_block, jnp.arange(BLOCKS, dtype=jnp.int32))
    return outputs.reshape(BLOCKS * BLOCK_TOKENS, QUERY_HEAD_COUNT * HEAD_SIZE)

def reference(tokens, norm_gain, w_query, key_projection_weight, value_projection_weight, w_out, counts):
    hidden = tokens
    token_positions = jnp.arange(SEQUENCE_TOKENS, dtype=jnp.int32)
    group_width = QUERY_HEAD_COUNT * HEAD_SIZE // N_HEAD
    for layer_position in range(LAYER_COUNT):
        normalized_rows = rms_norm(hidden, norm_gain[layer_position])
        queries = apply_rotary_embedding(jnp.dot(normalized_rows, w_query[layer_position], preferred_element_type=jnp.float32), token_positions, QUERY_HEAD_COUNT)
        key_rows_full = apply_rotary_embedding(jnp.dot(normalized_rows, key_projection_weight[layer_position], preferred_element_type=jnp.float32), token_positions, KEY_VALUE_HEADS)
        value_rows_full = jnp.dot(normalized_rows, value_projection_weight[layer_position], preferred_element_type=jnp.float32).astype(jnp.bfloat16).reshape(SEQUENCE_TOKENS, KEY_VALUE_HEADS, HEAD_SIZE)
        attended = attend(queries, key_rows_full, value_rows_full, counts)
        branch = jnp.zeros((SEQUENCE_TOKENS, MODEL_WIDTH), jnp.float32)
        for group_index in range(N_HEAD):
            column_start = group_index * group_width
            partial_product = jnp.dot(attended[:, column_start:column_start + group_width], w_out[layer_position, column_start:column_start + group_width], preferred_element_type=jnp.float32)
            rounded = lax.optimization_barrier(partial_product.astype(jnp.bfloat16))
            branch = branch + rounded.astype(jnp.float32)
        hidden = (hidden.astype(jnp.float32) + branch).astype(jnp.bfloat16)
    return hidden
```

```python
import functools
import math

import jax
import jax.numpy as jnp
from jax import lax
from jax.experimental import pallas as pl
from jax.experimental.pallas import tpu as pltpu
from jax.sharding import PartitionSpec as P

HEAD_SIZE = 128
WINDOW = 4096
PIECE = 128
FLAG_ROWS = 16
MESH = pl.DeviceIdType.MESH

norm_epsilon = 1e-05
rope_base = 10000.0
score_scale = math.log2(math.e) / math.sqrt(HEAD_SIZE)


def layers_kernel(
    sizes,
    counts_ref,
    tokens_ref,
    gain_ref,
    cosine_ref,
    sine_ref,
    wq_hbm,
    wk_hbm,
    wv_hbm,
    wo_hbm,
    out_ref,
    hidden,
    wq,
    wk,
    wv,
    wo,
    kv,
    flags,
    first_key,
    queries,
    scores,
    acc,
    top,
    attended,
    partial,
    theirs,
    kept_half,
    sent_half,
    their_half,
    weight_sem,
    token_sem,
    cross_send,
    cross_recv,
    kv_send,
    kv_recv,
):
    layer_total, rows, width, groups, group_length, span, blocks = sizes
    pieces = rows // PIECE
    heads = groups * group_length
    half = width // 2
    index = lax.axis_index("seq")
    head = lax.axis_index("head")
    pair = (index // 2) % 2
    core = index % 2
    own_half = pl.ds(pl.multiple_of(head * half, PIECE), half)
    other_half = pl.ds(pl.multiple_of((1 - head) * half, PIECE), half)
    across = {"head": 1 - head}

    def rows_of(c):
        return pl.ds(pl.multiple_of(c * PIECE, PIECE), PIECE)

    weights = [
        pltpu.make_async_copy(source.at[l], target.at[l], weight_sem.at[l, k])
        for l in range(layer_total)
        for k, (source, target) in enumerate(
            ((wk_hbm, wk), (wv_hbm, wv), (wq_hbm, wq), (wo_hbm, wo))
        )
    ]
    own_tokens = pltpu.make_async_copy(tokens_ref, hidden.at[:, own_half], token_sem)
    own_tokens.start()
    for copy in weights[:3]:
        copy.start()

    barrier = pltpu.get_barrier_semaphore()

    def greet(target):
        pl.semaphore_signal(barrier, inc=1, device_id=target, device_id_type=MESH)

    greet(across)
    greet({"seq": index + 2 - 4 * pair})
    greet({"seq": index + 1 - 2 * core})

    @pl.when(index + 4 < blocks)
    def _():
        greet({"seq": index + 4})

    @pl.when(index >= 4)
    def _():
        greet({"seq": index - 4})

    rounds = blocks // 4 - 1
    pl.semaphore_wait(
        barrier, 3 + jnp.minimum(index // 4, 1) + jnp.minimum(rounds - index // 4, 1)
    )

    def cross(source, target, stage, c):
        return pltpu.make_async_remote_copy(
            src_ref=source,
            dst_ref=target,
            send_sem=cross_send.at[stage, c],
            recv_sem=cross_recv.at[stage, c],
            device_id=across,
            device_id_type=MESH,
        )

    def token_copy(c):
        here = rows_of(c)
        return cross(tokens_ref.at[here], hidden.at[here, own_half], 0, c)

    def partial_copy(c):
        here = rows_of(c)
        return cross(partial.at[here], theirs.at[here], 1, c)

    def half_copy(c):
        here = rows_of(c)
        return cross(sent_half.at[here], their_half.at[here], 2, c)

    @pl.loop(0, pieces)
    def _(c):
        token_copy(c).start()

    for copy in weights[3:]:
        copy.start()

    lane_place = lax.broadcasted_iota(jnp.int32, (FLAG_ROWS, rows), 1)
    for d in range(span + 1):
        count = counts_ref[jnp.maximum(index - d, 0)]
        flags[d] = jnp.where(lane_place < count, 1.0, 0.0).astype(jnp.bfloat16)

    def step_of(d):
        if d % 4 == 0:
            return d - 4, index + 4, (index >= d - 4) & (index + 4 < blocks)
        if d % 2 == 0:
            source = d - 2 + 4 * pair
            return source, index + 2 - 4 * pair, index >= source
        source = d - 1 + 2 * core
        return source, index + 1 - 2 * core, index >= source

    def kv_copy(l, d, c):
        source, target, _ = step_of(d)
        if c is None:
            a, b, c = kv.at[l, source], kv.at[l, d], 0
        else:
            a, b = kv.at[l, source, c], kv.at[l, d, c]
        return pltpu.make_async_remote_copy(
            src_ref=a,
            dst_ref=b,
            send_sem=kv_send.at[l, d, c],
            recv_sem=kv_recv.at[l, d, c],
            device_id={"seq": target},
            device_id_type=MESH,
        )

    def send(l, d, c, also=True):
        @pl.when(step_of(d)[2] & also)
        def _():
            kv_copy(l, d, c).start()

    def landed(l, d, c, also=True):
        @pl.when((index >= d) & also)
        def _():
            kv_copy(l, d, c).wait_recv()

    def sent(l, d, c):
        @pl.when(step_of(d)[2])
        def _():
            kv_copy(l, d, c).wait_send()

    def pass_four(l, c):
        landed(l, 4, c)
        send(l, 8, c)
        send(l, 2, c, pair == 1)
        send(l, 6, c, pair == 0)

    def pass_eight(l, c):
        landed(l, 8, c)
        send(l, 6, c, pair == 1)

    def project(l, c):
        here = rows_of(c)
        widened = hidden[here, :].astype(jnp.float32)
        mean_square = jnp.mean(widened * widened, axis=1, keepdims=True)
        normed = (
            widened * lax.rsqrt(mean_square + norm_epsilon) * gain_ref[l : l + 1, :]
        ).astype(jnp.bfloat16)
        cosine, sine = cosine_ref[here, :], sine_ref[here, :]

        def rope(x):
            return x * cosine + pltpu.roll(x, HEAD_SIZE // 2, 1) * sine

        def lanes(x, h):
            return x[:, h * HEAD_SIZE : (h + 1) * HEAD_SIZE]

        valid = (
            lax.broadcasted_iota(jnp.int32, (PIECE, HEAD_SIZE), 0) + c * PIECE < counts_ref[index]
        )
        raw = jnp.dot(normed, wk[l], preferred_element_type=jnp.float32)
        for g in range(groups):
            key = rope(lanes(raw, g))

            @pl.when(c == 0)
            def _():
                first_key[g, 0:1, :] = key[0:1, :]

            key = jnp.where(valid, key, first_key[g, 0:1, :])
            kv[l, 0, c, 0, g] = key.astype(jnp.bfloat16)
        raw = jnp.dot(normed, wv[l], preferred_element_type=jnp.float32)
        for g in range(groups):
            value = jnp.where(valid, lanes(raw, g), 0.0)
            kv[l, 0, c, 1, g] = value.T.astype(jnp.bfloat16)

        @pl.when(c >= 1)
        def _():
            pass_four(l, c - 1)

        @pl.when(c >= 2)
        def _():
            pass_eight(l, c - 2)

        send(l, 4, c)
        send(l, 2, c, pair == 0)
        raw = jnp.dot(normed, wq[l], preferred_element_type=jnp.float32)
        for h in range(heads):
            query = rope(lanes(raw, h)) * score_scale
            queries[h * HEAD_SIZE : (h + 1) * HEAD_SIZE, here] = query.T.astype(jnp.bfloat16)

    key_place = lax.broadcasted_iota(jnp.int32, (rows, rows), 0)
    query_place = lax.broadcasted_iota(jnp.int32, (rows, rows), 1)

    def attend(l, first, stride, count, mask=None):
        steps = count * groups

        def score(i, h):
            slot, g = first + stride * (i // groups), i % groups
            keys = jnp.concatenate([kv[l, slot, c, 0, g] for c in range(pieces)], axis=0)
            at = pl.ds(pl.multiple_of((g * group_length + h) * HEAD_SIZE, HEAD_SIZE), HEAD_SIZE)
            s = jnp.dot(keys, queries[at, :], preferred_element_type=jnp.float32)
            if mask is not None:
                s = jnp.where(mask(), s, -jnp.inf)
            return s, jnp.max(s.reshape(rows // 8, 8, rows), axis=0)

        def keep(i, h, slot, pair_of):
            s, m = pair_of
            scores[slot] = s
            top[i % groups, 8:16, h * rows : (h + 1) * rows] = m

        @pl.when(steps > 0)
        def _():
            keep(0, 0, 0, score(0, 0))

        @pl.loop(0, steps)
        def _(i):
            slot, g = first + stride * (i // groups), i % groups
            values = jnp.concatenate([kv[l, slot, c, 1, g] for c in range(pieces)], axis=1)
            values = jnp.concatenate([values, flags[slot]], axis=0)
            for h in range(group_length):
                spot = slice(h * rows, (h + 1) * rows)
                if h + 1 < group_length:
                    at, following = i, h + 1
                else:
                    at, following = jnp.minimum(i + 1, steps - 1), 0
                new = score(at, following)
                before = top[g, 0:1, spot]
                after = jnp.maximum(before, jnp.max(top[g, 8:16, spot], axis=0, keepdims=True))
                probs = jnp.exp2(scores[h % 2] - after).astype(jnp.bfloat16)
                added = jnp.dot(values, probs, preferred_element_type=jnp.float32)
                acc[g, :, spot] = acc[g, :, spot] * jnp.exp2(before - after) + added
                top[g, 0:1, spot] = after
                keep(at, following, (h + 1) % 2, new)

    def after_or_at():
        return key_place <= query_place

    def inside_far():
        valid = key_place < counts_ref[jnp.maximum(index - span, 0)]
        return valid & (key_place > query_place)

    def present(first, stride, most):
        return jnp.clip((index - first) // stride + 1, 0, most)

    own_tokens.wait()
    for l in range(layer_total):
        last = l == layer_total - 1
        for copy in weights[4 * l : 4 * l + 3]:
            copy.wait()

        @pl.loop(0, pieces)
        def _(c):
            if l == 0:
                token_copy(c).wait_recv()
            else:
                partial_copy(c).wait_recv()
                here = rows_of(c)
                branch = partial[here, :].astype(jnp.float32) + theirs[here, :].astype(jnp.float32)
                hidden[here, :] = (hidden[here, :].astype(jnp.float32) + branch).astype(
                    jnp.bfloat16
                )
            project(l, c)

        send(l, 1, None, core == 0)
        acc[...] = jnp.zeros_like(acc)
        top[...] = jnp.full_like(top, -jnp.inf)
        attend(l, 0, 1, 1, after_or_at)
        pass_four(l, pieces - 1)
        send(l, 3, None, core == 1)
        send(l, 5, None, core == 0)
        pass_eight(l, pieces - 2)
        attend(l, 4, 1, present(4, 1, 1))
        pass_eight(l, pieces - 1)
        send(l, 7, None, core == 1)
        for c in range(pieces):
            landed(l, 2, c)
        send(l, 1, None, core == 1)
        send(l, 3, None, core == 0)
        attend(l, 8, 1, present(8, 1, 1), inside_far)
        landed(l, 1, None)
        landed(l, 3, None)
        attend(l, 1, 1, present(1, 1, 3))
        for c in range(pieces):
            landed(l, 6, c)
        send(l, 5, None, core == 1)
        send(l, 7, None, core == 0)
        attend(l, 6, 1, present(6, 1, 1))
        landed(l, 5, None)
        landed(l, 7, None)
        attend(l, 5, 2, present(5, 2, 2))

        @pl.loop(0, groups)
        def _(g):
            for h in range(group_length):
                spot = slice(h * rows, (h + 1) * rows)
                total = acc[g, HEAD_SIZE : HEAD_SIZE + 1, spot]
                result = acc[g, :HEAD_SIZE, spot] * (1.0 / total)
                at = pl.ds(pl.multiple_of((g * group_length + h) * HEAD_SIZE, HEAD_SIZE), HEAD_SIZE)
                attended[:, at] = result.T.astype(jnp.bfloat16)

        weights[4 * l + 3].wait()

        @pl.loop(0, pieces)
        def _(c):
            here = rows_of(c)
            if last:
                sent_half[here, :] = jnp.dot(
                    attended[here, :], wo[l, :, other_half], preferred_element_type=jnp.float32
                ).astype(jnp.bfloat16)
                half_copy(c).start()
                kept_half[here, :] = jnp.dot(
                    attended[here, :], wo[l, :, own_half], preferred_element_type=jnp.float32
                ).astype(jnp.bfloat16)
            else:
                partial[here, :] = jnp.dot(
                    attended[here, :], wo[l], preferred_element_type=jnp.float32
                ).astype(jnp.bfloat16)
                partial_copy(c).start()

    @pl.loop(0, pieces)
    def _(c):
        half_copy(c).wait_recv()
        here = rows_of(c)
        branch = kept_half[here, :].astype(jnp.float32) + their_half[here, :].astype(jnp.float32)
        out_ref[here, :] = (hidden[here, own_half].astype(jnp.float32) + branch).astype(
            jnp.bfloat16
        )

    @pl.loop(0, pieces)
    def _(c):
        token_copy(c).wait_send()
        partial_copy(c).wait_send()
        half_copy(c).wait_send()
        for l in range(layer_total):
            for d in (2, 4, 6, 8):
                sent(l, d, c)

    for l in range(layer_total):
        for d in (1, 3, 5, 7):
            sent(l, d, None)


def per_device(tokens, norm_gain, w_query, key_weight, value_weight, w_out, counts):
    rows, half = tokens.shape
    width = 2 * half
    layer_total = norm_gain.shape[0]
    span = WINDOW // rows
    pieces = rows // PIECE
    groups = key_weight.shape[2] // HEAD_SIZE
    heads = w_query.shape[2] // HEAD_SIZE
    group_length = heads // groups
    blocks = lax.axis_size("seq")
    assert span == 8 and blocks % 4 == 0 and layer_total == 2

    places = (lax.axis_index("seq") * rows + jnp.arange(rows, dtype=jnp.int32)).astype(jnp.float32)
    half_dim = HEAD_SIZE // 2
    inverse = jnp.power(
        jnp.float32(rope_base), -2.0 * jnp.arange(half_dim, dtype=jnp.float32) / HEAD_SIZE
    )
    angles = places[:, None] * inverse[None, :]
    cosine, sine = jnp.cos(angles), jnp.sin(angles)
    cosine = jnp.concatenate([cosine, cosine], axis=1)
    sine = jnp.concatenate([-sine, sine], axis=1)

    sizes = (layer_total, rows, width, groups, group_length, span, blocks)
    vmem = pl.BlockSpec(memory_space=pltpu.VMEM)
    smem = pl.BlockSpec(memory_space=pltpu.SMEM)
    anywhere = pl.BlockSpec(memory_space=pl.ANY)
    bf16, f32 = jnp.bfloat16, jnp.float32
    return pl.pallas_call(
        functools.partial(layers_kernel, sizes),
        out_shape=jax.ShapeDtypeStruct((rows, half), bf16),
        in_specs=[smem, anywhere, vmem, vmem, vmem] + [anywhere] * 4,
        out_specs=vmem,
        scratch_shapes=[
            pltpu.VMEM((rows, width), bf16),
            pltpu.VMEM(w_query.shape, bf16),
            pltpu.VMEM(key_weight.shape, bf16),
            pltpu.VMEM(value_weight.shape, bf16),
            pltpu.VMEM(w_out.shape, bf16),
            pltpu.VMEM((layer_total, span + 1, pieces, 2, groups, PIECE, HEAD_SIZE), bf16),
            pltpu.VMEM((span + 1, FLAG_ROWS, rows), bf16),
            pltpu.VMEM((groups, 8, HEAD_SIZE), f32),
            pltpu.VMEM((heads * HEAD_SIZE, rows), bf16),
            pltpu.VMEM((2, rows, rows), f32),
            pltpu.VMEM((groups, HEAD_SIZE + FLAG_ROWS, group_length * rows), f32),
            pltpu.VMEM((groups, 16, group_length * rows), f32),
            pltpu.VMEM((rows, heads * HEAD_SIZE), bf16),
            pltpu.VMEM((rows, width), bf16),
            pltpu.VMEM((rows, width), bf16),
            pltpu.VMEM((rows, half), bf16),
            pltpu.VMEM((rows, half), bf16),
            pltpu.VMEM((rows, half), bf16),
            pltpu.SemaphoreType.DMA((layer_total, 4)),
            pltpu.SemaphoreType.DMA,
            pltpu.SemaphoreType.DMA((3, pieces)),
            pltpu.SemaphoreType.DMA((3, pieces)),
            pltpu.SemaphoreType.DMA((layer_total, span + 1, pieces)),
            pltpu.SemaphoreType.DMA((layer_total, span + 1, pieces)),
        ],
        compiler_params=pltpu.CompilerParams(
            collective_id=0, has_side_effects=True, vmem_limit_bytes=63 * 1024 * 1024
        ),
        name="window_layers",
    )(counts, tokens, norm_gain, cosine, sine, w_query, key_weight, value_weight, w_out)


def solution(mesh):
    return jax.shard_map(
        per_device,
        mesh=mesh,
        in_specs=(
            P("seq", "head"),
            P(),
            P(None, None, "head"),
            P(None, None, "head"),
            P(None, None, "head"),
            P(None, "head", None),
            P(),
        ),
        out_specs=P("seq", "head"),
        check_vma=False,
    )
```
